32 devices in a mesh: expert: 4 (over z), tensor: 8 (over y, x, core).
Axes of the slice: x: 2, y: 2, z: 4, core: 2. Of those that a mesh axis runs over, the one named last changes fastest.
Arguments:
- stashed: bfloat16 [384, 4096], P('expert', 'tensor'), may hold values from -6 to 6
- expert_ids: int32 [384, 2], P('expert'), may hold values from 0 to 3, all different within a row; in each aligned block of 96 rows (0 to 95, 96 to 191, ...) at most 64 rows name the same one
- combine_weight: float32 [384, 2], P('expert'), may hold values from 0.2 to 1
- w_gate: bfloat16 [4, 7168, 4096], P('expert', 'tensor'), may hold values from -0.09375 to 0.09375
- w_up: bfloat16 [4, 7168, 4096], P('expert', 'tensor'), may hold values from -0.09375 to 0.09375
- w_down: bfloat16 [4, 7168, 4096], P('expert', 'tensor'), may hold values from -0.09375 to 0.09375
Outputs:
- mixed_out: bfloat16 [384, 4096], P('expert', 'tensor')
The draws below stay inside these ranges and needn't reach their ends.
Inputs may be any that keep to these rules, and one draw needn't show every extreme that they name: `expert_ids`: each row names two different experts. Among the 96 rows of one group (aligned blocks) no expert is named more than 64 times, and in some group some expert is named exactly 64 times.
All inputs are finite; a program needn't handle non-finite values.
Results may differ from the reference program's by a relative error of at most 0.0049.
Values may be sent and summed in bfloat16 or wider, within the bound.
A program may use at most 64 MiB of HBM per device.

```python
import math
import jax
import jax.numpy as jnp
import numpy as np
from jax import lax

D = 4096
FF = 7168
TOK_E = 96
EXPERTS = 4
TOKENS = 384
CAP = 64


def spiked(values, stream_key, source, target, blocks, factor):
    def block_of(position):
        return (jnp.arange(values.shape[position]) // (values.shape[position] // blocks)).reshape((-1,) + (1,) * (values.ndim - 1 - position))

    one_side = jax.random.permutation(stream_key, blocks)[block_of(target)]
    far = (block_of(target) + blocks // 2) % blocks
    return jnp.where((block_of(source) == one_side) | (block_of(source) == far), factor * values, values)


def block_levels(key, extent, pieces, low, top_value):
    def one(axis_at, shards_of):
        draws = jax.random.uniform(jax.random.fold_in(jax.random.fold_in(key, 6), axis_at), (shards_of,), jnp.float32, low / len(pieces), top_value / len(pieces))
        return jnp.repeat(jnp.exp(draws), extent[axis_at] // shards_of).reshape((-1,) + (1,) * (len(extent) - axis_at - 1))

    level = one(*pieces[0])
    for cut in pieces[1:]:
        level = level * one(*cut)
    return level


def shared_out(key, own, number, rows, number_of, top, limit, skew):
    ranking = jax.random.permutation(key, number_of)
    crowded, common = load_shares(number_of, rows * top, limit, skew, True), load_shares(number_of, rows * top, limit, skew, False)
    places = jnp.arange(number_of)

    def named(tallies, turn):
        used = int((tallies > 0).sum())
        fixed = max(1, used // 4)
        shifted = fixed + (places - fixed + turn * (used - fixed)) % max(1, number_of - fixed)
        return jnp.zeros((number_of,), jnp.int32).at[ranking[jnp.where(places < fixed, places, shifted)]].set(jnp.asarray(tallies, jnp.int32))

    tallies = jnp.where(number % 4 == 0, named(crowded, number // 4), named(common, number - number // 4 - 1))
    mixed = jax.random.permutation(jax.random.fold_in(own, 3), number_of)
    donor, sink = mixed[0:number_of // 2 * 2:2], mixed[1:number_of // 2 * 2:2]
    room = jnp.minimum(tallies[donor] - 1, limit - tallies[sink]) // 2
    room = jnp.where((donor == ranking[0]) | (sink == ranking[0]) | (tallies[sink] == 0), 0, jnp.maximum(room, 0))
    shifted = jax.random.randint(jax.random.fold_in(own, 4), (number_of // 2,), 0, 1 << 20) % (room + 1)
    tallies = tallies.at[donor].add(-shifted).at[sink].add(shifted)
    items = jnp.searchsorted(jnp.cumsum(tallies), jnp.arange(rows * top), side="right").astype(jnp.int32)
    grid = items.reshape(top, rows).T
    grid = grid[jax.random.permutation(jax.random.fold_in(own, 1), rows)]
    turn = jax.random.randint(jax.random.fold_in(own, 2), (rows, 1), 0, top)
    return jnp.take_along_axis(grid, (jnp.arange(top)[None, :] + turn) % top, axis=1)


def load_shares(number_of, total, bound, lean, full):
    loads = [(1 << 20) // math.isqrt(standing ** lean) + 1 for standing in range(1, number_of + 1)]
    largest = bound if full else min(bound, max(-(-total // number_of), total * loads[0] // sum(loads)))
    least = 1 if total - largest >= number_of - 1 else 0
    counts, spare = [largest] + [least] * (number_of - 1), total - largest - least * (number_of - 1)
    while spare > 0:
        movable = [i for i in range(1, number_of) if counts[i] < largest] or [i for i in range(1, number_of) if counts[i] < bound]
        pool, left = sum([loads[i] for i in movable]), spare
        for i in movable:
            more = min(bound - counts[i], max(1, left * loads[i] // pool), spare)
            counts[i] = counts[i] + more
            spare = spare - more
    return np.array(counts)


def normal_values(key, extent, scale, bound, pieces=(), kind=jnp.bfloat16):
    entries = scale * jax.random.normal(key, extent, jnp.float32)
    if pieces:
        entries = entries * block_levels(key, extent, pieces, -0.22, 0.18)
    return jnp.clip(entries, -bound, bound).astype(kind)


def heavy_noise(stream_key, extent, scale, limit, cuts, heavy, kind=jnp.bfloat16):
    entries = scale * jax.random.normal(stream_key, extent, jnp.float32)
    if cuts:
        entries = entries * block_levels(stream_key, extent, cuts, -0.22, 0.18)
    return jnp.clip(spiked(entries, jax.random.fold_in(stream_key, 3), *heavy), -limit, limit).astype(kind)


def setup_inputs(seed: int = 0) -> dict:
    key_of = jax.random.split(jax.random.key(seed), 7)
    stashed = normal_values(key_of[0], (TOKENS, D), 1.0, 6.0, ((0, 4), (1, 8)))
    expert_ids_keys = jax.random.split(jax.random.fold_in(key_of[1], 1), TOKENS // TOK_E)
    expert_ids_turns = jax.random.permutation(jax.random.fold_in(key_of[1], 3), TOKENS // TOK_E)
    expert_ids = jax.vmap(lambda own, number: shared_out(jax.random.fold_in(key_of[1], 2), own, number, TOK_E, EXPERTS, 2, CAP, 2))(expert_ids_keys, expert_ids_turns).reshape((TOKENS, 2))
    combine_weight = jnp.clip(0.2 + 0.8 * jax.random.uniform(key_of[2], (TOKENS, 2), jnp.float32) ** block_levels(key_of[2], (TOKENS, 2), ((0, 4),), -0.2, 0.2), 0.2, 1.0)
    w_gate = normal_values(key_of[3], (EXPERTS, FF, D), D ** -0.5, 0.09375, ((0, 4), (1, 8)))
    w_up = normal_values(key_of[4], (EXPERTS, FF, D), D ** -0.5, 0.09375, ((0, 4), (1, 8)))
    w_down = heavy_noise(key_of[5], (EXPERTS, FF, D), FF ** -0.5, 0.09375, ((0, 4), (1, 8)), (1, 2, 8, 2.0))
    return dict(stashed=stashed, expert_ids=expert_ids, combine_weight=combine_weight, w_gate=w_gate, w_up=w_up, w_down=w_down)


def slot_targets(expert_ids, experts, capacity):
    flat_ids = expert_ids.reshape(-1)
    one_hot = (flat_ids[:, None] == jnp.arange(experts, dtype=jnp.int32)[None, :]).astype(jnp.int32)
    before = jnp.cumsum(one_hot, axis=0) - one_hot
    slot_index = jnp.sum(before * one_hot, axis=1)
    return (flat_ids * capacity + slot_index).astype(jnp.int32).reshape(expert_ids.shape)


def contract_last(left, right):
    return lax.dot_general(left, right, (((1,), (1,)), ((), ())), preferred_element_type=jnp.float32)


def reference(stashed, expert_ids, combine_weight, w_gate, w_up, w_down):
    groups = stashed.shape[0] // TOK_E
    width = stashed.shape[1]
    grouped_ids = expert_ids.reshape(groups, TOK_E, 2)
    targets = jax.vmap(lambda ids: slot_targets(ids, EXPERTS, CAP))(grouped_ids)
    grouped_tokens = stashed.reshape(groups, TOK_E, width)
    values = jnp.broadcast_to(grouped_tokens[:, :, None, :], (groups, TOK_E, 2, width))
    group_index = jnp.broadcast_to(jnp.arange(groups, dtype=jnp.int32)[:, None, None], targets.shape)
    buffer = jnp.zeros((groups, EXPERTS * CAP, width), jnp.bfloat16)
    buffer = buffer.at[group_index, targets].set(values)
    buffer = buffer.reshape(groups, EXPERTS, CAP, width).transpose(1, 0, 2, 3).reshape(EXPERTS, groups * CAP, width)

    def expert_layer(operands):
        rows_in, gate_w, up_w, down_w = operands
        gate_acts = contract_last(rows_in, gate_w)
        up_acts = contract_last(rows_in, up_w)
        hidden = (jax.nn.silu(gate_acts) * up_acts).astype(jnp.bfloat16)
        return jnp.dot(hidden, down_w, preferred_element_type=jnp.float32)

    expert_out = lax.map(expert_layer, (buffer, w_gate, w_up, w_down))
    expert_out = expert_out.reshape(EXPERTS, groups, CAP, width).transpose(1, 0, 2, 3).reshape(groups, EXPERTS * CAP, width)
    gathered_out = expert_out[group_index, targets]
    weights = combine_weight.reshape(groups, TOK_E, 2)
    mixed_out = jnp.sum(weights[:, :, :, None] * gathered_out, axis=2)
    return mixed_out.reshape(groups * TOK_E, width).astype(jnp.bfloat16)
```

```python
import functools

import jax
import jax.numpy as jnp
from jax import lax
from jax.experimental import pallas as pl
from jax.experimental.pallas import tpu as pltpu
from jax.sharding import PartitionSpec as P


def slot_targets(expert_ids, experts, capacity):
    flat_ids = expert_ids.reshape(-1)
    one_hot = (flat_ids[:, None] == jnp.arange(experts, dtype=jnp.int32)[None, :]).astype(jnp.int32)
    before = jnp.cumsum(one_hot, axis=0) - one_hot
    slot_index = jnp.sum(before * one_hot, axis=1)
    return (flat_ids * capacity + slot_index).reshape(expert_ids.shape)


def contract_last(left, right):
    return lax.dot_general(
        left, right, (((1,), (1,)), ((), ())), preferred_element_type=jnp.float32
    )


def shards(stashed, expert_ids, combine_weight, w_gate, w_up, w_down):
    tok_count = stashed.shape[0]
    feat_width = stashed.shape[1]
    experts = lax.axis_size("expert")
    capacity = min(tok_count, 8 * tok_count // (3 * experts))
    targets = slot_targets(expert_ids, experts, capacity)
    columns = jnp.arange(experts * capacity, dtype=jnp.int32)
    pair_match = (targets[:, :, None] == columns[None, None, :]).astype(jnp.float32)
    selector = jnp.sum(pair_match, axis=1).T.astype(jnp.bfloat16)
    mixing = jnp.sum(pair_match * combine_weight[:, :, None], axis=1)
    gate_w = w_gate[0]
    up_w = w_up[0]
    down_w = w_down[0]
    gathered = lax.all_gather(stashed, "tensor", axis=1, tiled=True)
    outgoing = jnp.dot(selector, gathered, preferred_element_type=jnp.float32).astype(jnp.bfloat16)
    outgoing = outgoing.reshape(experts, capacity, gathered.shape[1])
    received = lax.all_to_all(outgoing, "expert", split_axis=0, concat_axis=0, tiled=True)
    sources, item_count, full_width = received.shape
    rows_in = received.reshape(sources * item_count, full_width)
    gate_acts = contract_last(rows_in, gate_w)
    up_acts = contract_last(rows_in, up_w)
    hidden = (jax.nn.silu(gate_acts) * up_acts).astype(jnp.bfloat16)
    result = jnp.dot(hidden, down_w, preferred_element_type=jnp.float32)
    partial_value = result.reshape(sources, item_count, result.shape[1])
    partial_value = partial_value.reshape(-1, partial_value.shape[2])
    own_share = lax.psum_scatter(partial_value, "tensor", scatter_dimension=1, tiled=True)
    returned_rows = lax.all_to_all(
        own_share.reshape(experts, capacity, feat_width),
        "expert",
        split_axis=0,
        concat_axis=0,
        tiled=True,
    )
    combined = jnp.dot(
        mixing,
        returned_rows.reshape(experts * capacity, feat_width),
        precision=lax.Precision.HIGHEST,
        preferred_element_type=jnp.float32,
    )
    return combined.astype(jnp.bfloat16)


MESH = pl.DeviceIdType.MESH


def flip(index, bit):
    return index + bit - 2 * bit * lax.rem(lax.div(index, bit), 2)


def layer_kernel(
    groups, cap,
    x_ref, ids_ref, cw_ref, wg_hbm, wu_hbm, wd_hbm, out_ref,
    wg, wu, wd, picked, rows_in, gate_acc, up_acc, hidden,
    sib_out, sib_in, own_part, d_out, d_in, x_out, x_in, y_out, y_in, z_out, z_in,
    w_sem, send_sem, recv_sem,
):
    tokens, feat = x_ref.shape
    z = lax.axis_index("expert")
    t = lax.axis_index("tensor")
    sib, tx, ty = flip(t, 1), flip(t, 2), flip(t, 4)
    td = flip(tx, 4)
    group_of = [z, flip(z, 1), flip(z, 2), flip(flip(z, 1), 2)]
    steps = range(groups)

    loads = []
    for i, (hbm, vmem) in enumerate(((wg_hbm, wg), (wu_hbm, wu), (wd_hbm, wd))):
        half = vmem.shape[0] // 2
        for j in range(2):
            part = pl.ds(j * half, half)
            loads.append(pltpu.make_async_copy(hbm.at[0, part], vmem.at[part], w_sem.at[2 * i + j]))
    for load in loads:
        load.start()

    barrier = pltpu.get_barrier_semaphore()
    peers = [{"tensor": sib}, {"tensor": tx}, {"tensor": ty}]
    peers += [{"expert": group_of[s]} for s in steps[1:]]
    for peer in peers:
        pl.semaphore_signal(barrier, inc=1, device_id=peer, device_id_type=MESH)

    ids = ids_ref[...]
    lanes = lax.broadcasted_iota(jnp.int32, (tokens, 128), 1)
    first = (ids[:, 0:1] == lanes).astype(jnp.float32)
    second = (ids[:, 1:2] == lanes).astype(jnp.float32)
    earlier = (
        lax.broadcasted_iota(jnp.int32, (tokens, tokens), 1)
        < lax.broadcasted_iota(jnp.int32, (tokens, tokens), 0)
    ).astype(jnp.bfloat16)
    before = jnp.dot(earlier, (first + second).astype(jnp.bfloat16), preferred_element_type=jnp.float32)
    slot0 = jnp.sum(before * first, axis=1, keepdims=True)
    slot1 = jnp.sum((before + first) * second, axis=1, keepdims=True)
    place = (ids ^ z).astype(jnp.float32) * cap
    columns = lax.broadcasted_iota(jnp.int32, (tokens, groups * cap), 1).astype(jnp.float32)
    match0 = (columns == place[:, 0:1] + slot0).astype(jnp.float32)
    match1 = (columns == place[:, 1:2] + slot1).astype(jnp.float32)
    selector = (match0 + match1).astype(jnp.bfloat16)
    picked[...] = lax.dot_general(
        selector, x_ref[...], (((0,), (0,)), ((), ())), preferred_element_type=jnp.float32
    ).astype(jnp.bfloat16)

    def group_rows(s):
        return pl.ds(pl.multiple_of(group_of[s] * cap, cap), cap)

    def block(owner, s):
        lanes_at = pl.ds(pl.multiple_of(lax.rem(owner, 2) * feat, feat), feat)
        return rows_in.at[lax.div(owner, 2), group_rows(s), lanes_at]

    copies = {}

    def send(name, s, src, dst, peer):
        number = NAMES.index(name) * groups + s
        copy = pltpu.make_async_remote_copy(
            src_ref=src, dst_ref=dst, send_sem=send_sem.at[number], recv_sem=recv_sem.at[number],
            device_id=peer, device_id_type=MESH,
        )
        copy.start()
        copies[name, s] = copy

    def arrive(name, s):
        copies[name, s].wait_recv()

    own_at = block(t, 0)
    own_at[...] = picked[pl.ds(0, cap)]
    pl.semaphore_wait(barrier, len(peers))

    def share(s):
        here = block(t, s)
        send("own_x", s, here, here, {"tensor": tx})
        send("own_y", s, here, here, {"tensor": ty})
        send("own_sib", s, here, here, {"tensor": sib})

    def pass_x(s):
        arrive("own_x", s)
        here = block(tx, s)
        if s % 2 == 0:
            send("diag", s, here, here, {"tensor": ty})
        send("sib_x", s, here, here, {"tensor": sib})

    def pass_y(s):
        arrive("own_y", s)
        here = block(ty, s)
        if s % 2 == 1:
            send("diag", s, here, here, {"tensor": tx})
        send("sib_y", s, here, here, {"tensor": sib})

    def pass_diag(s):
        arrive("diag", s)
        here = block(td, s)
        send("sib_d", s, here, here, {"tensor": sib})

    def project(owner, start):
        pair = lax.div(owner, 2)
        rows = rows_in[pair]
        lanes_at = pl.ds(pl.multiple_of(pair * (2 * feat), 2 * feat), 2 * feat)
        for weight, acc in ((wg, gate_acc), (wu, up_acc)):
            part = contract_last(rows, weight[:, lanes_at])
            acc[...] = part if start else acc[...] + part

    for s in (3, 2, 1):
        send("z", s, picked.at[pl.ds(s * cap, cap)], block(t, 0), {"expert": group_of[s]})
    share(0)
    arrive("z", 1)
    share(1)
    pass_x(0)
    pass_y(0)
    arrive("z", 2)
    share(2)
    arrive("z", 3)
    share(3)
    pass_x(1)
    pass_y(1)
    for load in loads[:4]:
        load.wait()
    for s in steps:
        arrive("own_sib", s)
    project(t, True)
    pass_x(2)
    pass_y(2)
    pass_diag(0)
    pass_diag(1)
    pass_x(3)
    pass_y(3)
    for s in steps:
        arrive("sib_x", s)
    project(tx, False)
    pass_diag(2)
    pass_diag(3)
    for s in steps:
        arrive("sib_y", s)
    project(ty, False)
    for s in steps:
        arrive("sib_d", s)
    project(td, False)
    gate = gate_acc[...]
    hidden[...] = (gate / (1.0 + jnp.exp(-gate)) * up_acc[...]).astype(jnp.bfloat16)
    for load in loads[4:]:
        load.wait()

    owners = (t, tx, ty, td)

    def down(owner):
        lanes_at = pl.ds(pl.multiple_of(owner * feat, feat), feat)
        return jnp.dot(hidden[...], wd[:, lanes_at], preferred_element_type=jnp.float32)

    def partial_sums(q):
        sib_out[q] = down(flip(owners[q], 1)).astype(jnp.bfloat16)
        send("sum_sib", q, sib_out.at[q], sib_in.at[q], {"tensor": sib})
        own_part[q] = down(owners[q])

    def chip_sum(q, s):
        at = group_rows(s)
        return own_part[q, at] + sib_in[q, at].astype(jnp.float32)

    def sum_d(s):
        d_out[s] = chip_sum(3, s).astype(jnp.bfloat16)
        send("sum_d", s, d_out.at[s], d_in.at[s], {"tensor": tx if s % 2 == 0 else ty})

    def sum_x(s):
        value = chip_sum(1, s)
        if s % 2 == 1:
            arrive("sum_d", s)
            value = value + d_in[s].astype(jnp.float32)
        x_out[s] = value.astype(jnp.bfloat16)
        send("sum_x", s, x_out.at[s], x_in.at[s], {"tensor": tx})

    def sum_y(s):
        value = chip_sum(2, s)
        if s % 2 == 0:
            arrive("sum_d", s)
            value = value + d_in[s].astype(jnp.float32)
        y_out[s] = value.astype(jnp.bfloat16)
        send("sum_y", s, y_out.at[s], y_in.at[s], {"tensor": ty})

    def total(s):
        arrive("sum_x", s)
        arrive("sum_y", s)
        value = chip_sum(0, s) + x_in[s].astype(jnp.float32) + y_in[s].astype(jnp.float32)
        return value.astype(jnp.bfloat16)

    def give_back(s):
        z_out[s] = total(s)
        send("back", s, z_out.at[s], z_in.at[pl.ds(s * cap, cap)], {"expert": group_of[s]})

    partial_sums(3)
    partial_sums(1)
    arrive("sum_sib", 3)
    sum_d(2)
    sum_d(3)
    partial_sums(2)
    arrive("sum_sib", 1)
    sum_x(2)
    arrive("sum_sib", 2)
    sum_y(3)
    sum_d(0)
    sum_d(1)
    partial_sums(0)
    sum_x(3)
    sum_y(2)
    sum_x(0)
    sum_y(1)
    arrive("sum_sib", 0)
    give_back(2)
    give_back(3)
    sum_x(1)
    sum_y(0)
    give_back(1)
    z_in[pl.ds(0, cap)] = total(0)

    weights = cw_ref[...]
    mixing = match0 * weights[:, 0:1] + match1 * weights[:, 1:2]
    coarse = mixing.astype(jnp.bfloat16)
    fine = (mixing - coarse.astype(jnp.float32)).astype(jnp.bfloat16)
    for s in (2, 3, 1):
        arrive("back", s)
    returned = z_in[...]
    combined = jnp.dot(coarse, returned, preferred_element_type=jnp.float32)
    combined += jnp.dot(fine, returned, preferred_element_type=jnp.float32)
    out_ref[...] = combined.astype(jnp.bfloat16)
    for copy in copies.values():
        copy.wait_send()


NAMES = (
    "z", "own_x", "own_y", "own_sib", "diag", "sib_x", "sib_y", "sib_d",
    "sum_sib", "sum_d", "sum_x", "sum_y", "back",
)


def fused_shards(stashed, expert_ids, combine_weight, w_gate, w_up, w_down):
    groups = lax.axis_size("expert")
    tokens, feat = stashed.shape
    cap = min(tokens, 8 * tokens // (3 * groups))
    _, units, width = w_gate.shape
    rows = groups * cap
    bf16, f32 = jnp.bfloat16, jnp.float32
    vmem = pl.BlockSpec(memory_space=pltpu.VMEM)
    hbm = pl.BlockSpec(memory_space=pl.ANY)
    pieces = [pltpu.VMEM((groups, cap, feat), bf16)] * 7
    return pl.pallas_call(
        functools.partial(layer_kernel, groups, cap),
        out_shape=jax.ShapeDtypeStruct((tokens, feat), bf16),
        in_specs=[vmem, vmem, vmem, hbm, hbm, hbm],
        out_specs=vmem,
        scratch_shapes=[
            pltpu.VMEM((units, width), bf16),
            pltpu.VMEM((units, width), bf16),
            pltpu.VMEM((units, width), bf16),
            pltpu.VMEM((rows, feat), bf16),
            pltpu.VMEM((width // (2 * feat), rows, 2 * feat), bf16),
            pltpu.VMEM((rows, units), f32),
            pltpu.VMEM((rows, units), f32),
            pltpu.VMEM((rows, units), bf16),
            pltpu.VMEM((4, rows, feat), bf16),
            pltpu.VMEM((4, rows, feat), bf16),
            pltpu.VMEM((4, rows, feat), f32),
            *pieces,
            pltpu.VMEM((rows, feat), bf16),
            pltpu.SemaphoreType.DMA((6,)),
            pltpu.SemaphoreType.DMA((len(NAMES) * groups,)),
            pltpu.SemaphoreType.DMA((len(NAMES) * groups,)),
        ],
        compiler_params=pltpu.CompilerParams(
            collective_id=0, has_side_effects=True, vmem_limit_bytes=60 * 1024 * 1024
        ),
    )(stashed, expert_ids, combine_weight, w_gate, w_up, w_down)


def picks_kernel(mesh):
    return mesh.shape["tensor"] == 8 and mesh.shape["expert"] == 4


def solution(mesh):
    return jax.shard_map(
        fused_shards if picks_kernel(mesh) else shards,
        mesh=mesh,
        in_specs=(
            P("expert", "tensor"),
            P("expert", None),
            P("expert", None),
            P("expert", "tensor", None),
            P("expert", "tensor", None),
            P("expert", "tensor", None),
        ),
        out_specs=P("expert", "tensor"),
        check_vma=False,
    )
```

```python
import functools

import jax
import jax.numpy as jnp
from jax import lax
from jax.experimental import pallas as pl
from jax.experimental.pallas import tpu as pltpu
from jax.sharding import PartitionSpec as P


def slot_targets(expert_ids, experts, capacity):
    flat_ids = expert_ids.reshape(-1)
    one_hot = (flat_ids[:, None] == jnp.arange(experts, dtype=jnp.int32)[None, :]).astype(jnp.int32)
    before = jnp.cumsum(one_hot, axis=0) - one_hot
    slot_index = jnp.sum(before * one_hot, axis=1)
    return (flat_ids * capacity + slot_index).reshape(expert_ids.shape)


def contract_last(left, right):
    return lax.dot_general(
        left, right, (((1,), (1,)), ((), ())), preferred_element_type=jnp.float32
    )


def contract_first(left, right):
    return lax.dot_general(
        left, right, (((0,), (0,)), ((), ())), preferred_element_type=jnp.float32
    )


def shards(stashed, expert_ids, combine_weight, w_gate, w_up, w_down):
    tok_count = stashed.shape[0]
    feat_width = stashed.shape[1]
    experts = lax.axis_size("expert")
    capacity = min(tok_count, 8 * tok_count // (3 * experts))
    targets = slot_targets(expert_ids, experts, capacity)
    columns = jnp.arange(experts * capacity, dtype=jnp.int32)
    pair_match = (targets[:, :, None] == columns[None, None, :]).astype(jnp.float32)
    selector = jnp.sum(pair_match, axis=1).T.astype(jnp.bfloat16)
    mixing = jnp.sum(pair_match * combine_weight[:, :, None], axis=1)
    gate_w = w_gate[0]
    up_w = w_up[0]
    down_w = w_down[0]
    gathered = lax.all_gather(stashed, "tensor", axis=1, tiled=True)
    outgoing = jnp.dot(selector, gathered, preferred_element_type=jnp.float32).astype(jnp.bfloat16)
    outgoing = outgoing.reshape(experts, capacity, gathered.shape[1])
    received = lax.all_to_all(outgoing, "expert", split_axis=0, concat_axis=0, tiled=True)
    sources, item_count, full_width = received.shape
    rows_in = received.reshape(sources * item_count, full_width)
    gate_acts = contract_last(rows_in, gate_w)
    up_acts = contract_last(rows_in, up_w)
    hidden = (jax.nn.silu(gate_acts) * up_acts).astype(jnp.bfloat16)
    result = jnp.dot(hidden, down_w, preferred_element_type=jnp.float32)
    partial_value = result.reshape(sources, item_count, result.shape[1])
    partial_value = partial_value.reshape(-1, partial_value.shape[2])
    own_share = lax.psum_scatter(partial_value, "tensor", scatter_dimension=1, tiled=True)
    returned_rows = lax.all_to_all(
        own_share.reshape(experts, capacity, feat_width),
        "expert",
        split_axis=0,
        concat_axis=0,
        tiled=True,
    )
    combined = jnp.dot(
        mixing,
        returned_rows.reshape(experts * capacity, feat_width),
        precision=lax.Precision.HIGHEST,
        preferred_element_type=jnp.float32,
    )
    return combined.astype(jnp.bfloat16)


MESH = pl.DeviceIdType.MESH


def flip(index, bit):
    return index + bit - 2 * bit * lax.rem(lax.div(index, bit), 2)


def layer_kernel(
    groups, cap,
    x_ref, ids_ref, cw_ref, wg_hbm, wu_hbm, wd_hbm, out_ref,
    wg, wu, wd, picked, rows_in, gate_acc, up_acc, hidden,
    sib_out, sib_in, own_part, d_out, d_in, x_out, x_in, y_out, y_in, z_out, z_in,
    w_sem, send_sem, recv_sem,
):
    tokens, feat = x_ref.shape
    z = lax.axis_index("expert")
    t = lax.axis_index("tensor")
    sib, tx, ty = flip(t, 1), flip(t, 2), flip(t, 4)
    td = flip(tx, 4)
    group_of = [z, flip(z, 1), flip(z, 2), flip(flip(z, 1), 2)]
    steps = range(groups)

    loads = []
    for i, (hbm, vmem) in enumerate(((wg_hbm, wg), (wu_hbm, wu), (wd_hbm, wd))):
        half = vmem.shape[0] // 2
        for j in range(2):
            part = pl.ds(j * half, half)
            loads.append(pltpu.make_async_copy(hbm.at[0, part], vmem.at[part], w_sem.at[2 * i + j]))
    for load in loads:
        load.start()

    barrier = pltpu.get_barrier_semaphore()
    peers = [{"tensor": sib}, {"tensor": tx}, {"tensor": ty}]
    peers += [{"expert": group_of[s]} for s in steps[1:]]
    for peer in peers:
        pl.semaphore_signal(barrier, inc=1, device_id=peer, device_id_type=MESH)

    ids = ids_ref[...]
    experts_at = lax.broadcasted_iota(jnp.int32, (8, tokens), 0)
    first = (ids[0:1] == experts_at).astype(jnp.float32)
    second = (ids[1:2] == experts_at).astype(jnp.float32)
    earlier = (
        lax.broadcasted_iota(jnp.int32, (tokens, tokens), 0)
        < lax.broadcasted_iota(jnp.int32, (tokens, tokens), 1)
    ).astype(jnp.bfloat16)
    before = jnp.dot((first + second).astype(jnp.bfloat16), earlier, preferred_element_type=jnp.float32)
    slot0 = jnp.sum(before * first, axis=0, keepdims=True)
    slot1 = jnp.sum((before + first) * second, axis=0, keepdims=True)
    place = (ids ^ z).astype(jnp.float32) * cap
    slots = lax.broadcasted_iota(jnp.int32, (groups * cap, tokens), 0).astype(jnp.float32)
    match0 = (slots == place[0:1] + slot0).astype(jnp.float32)
    match1 = (slots == place[1:2] + slot1).astype(jnp.float32)
    selector = (match0 + match1).astype(jnp.bfloat16)
    picked[...] = jnp.dot(selector, x_ref[...], preferred_element_type=jnp.float32).astype(jnp.bfloat16)

    def group_rows(s):
        return pl.ds(pl.multiple_of(group_of[s] * cap, cap), cap)

    def block(owner, s):
        lanes_at = pl.ds(pl.multiple_of(lax.rem(owner, 2) * feat, feat), feat)
        return rows_in.at[lax.div(owner, 2), group_rows(s), lanes_at]

    copies = {}

    def send(name, s, src, dst, peer):
        number = NAMES.index(name) * groups + s
        copy = pltpu.make_async_remote_copy(
            src_ref=src, dst_ref=dst, send_sem=send_sem.at[number], recv_sem=recv_sem.at[number],
            device_id=peer, device_id_type=MESH,
        )
        copy.start()
        copies[name, s] = copy

    def arrive(name, s):
        copies[name, s].wait_recv()

    own_at = block(t, 0)
    own_at[...] = picked[pl.ds(0, cap)]
    pl.semaphore_wait(barrier, len(peers))

    def share(s):
        here = block(t, s)
        send("own_x", s, here, here, {"tensor": tx})
        send("own_y", s, here, here, {"tensor": ty})
        send("own_sib", s, here, here, {"tensor": sib})

    def pass_x(s):
        arrive("own_x", s)
        here = block(tx, s)
        if s % 2 == 0:
            send("diag", s, here, here, {"tensor": ty})
        send("sib_x", s, here, here, {"tensor": sib})

    def pass_y(s):
        arrive("own_y", s)
        here = block(ty, s)
        if s % 2 == 1:
            send("diag", s, here, here, {"tensor": tx})
        send("sib_y", s, here, here, {"tensor": sib})

    def pass_diag(s):
        arrive("diag", s)
        here = block(td, s)
        send("sib_d", s, here, here, {"tensor": sib})

    def project(owner, start):
        pair = lax.div(owner, 2)
        rows = rows_in[pair]
        lanes_at = pl.ds(pl.multiple_of(pair * (2 * feat), 2 * feat), 2 * feat)
        for weight, acc in ((wg, gate_acc), (wu, up_acc)):
            part = contract_last(rows, weight[:, lanes_at])
            acc[...] = part if start else acc[...] + part

    for s in (1, 2, 3):
        send("z", s, picked.at[pl.ds(s * cap, cap)], block(t, 0), {"expert": group_of[s]})
    share(0)
    arrive("z", 1)
    share(1)
    pass_x(0)
    pass_y(0)
    pass_x(1)
    pass_y(1)
    arrive("z", 2)
    share(2)
    arrive("z", 3)
    share(3)
    pass_diag(0)
    pass_diag(1)
    for load in loads[:4]:
        load.wait()
    for s in steps:
        arrive("own_sib", s)
    project(t, True)
    pass_x(2)
    pass_y(2)
    pass_x(3)
    pass_y(3)
    for s in steps:
        arrive("sib_x", s)
    project(tx, False)
    pass_diag(2)
    pass_diag(3)
    for s in steps:
        arrive("sib_y", s)
    project(ty, False)
    for s in steps:
        arrive("sib_d", s)
    project(td, False)
    gate = gate_acc[...]
    hidden[...] = (gate / (1.0 + jnp.exp(-gate)) * up_acc[...]).astype(jnp.bfloat16)
    for load in loads[4:]:
        load.wait()

    owners = (t, tx, ty, td)

    def down(owner):
        lanes_at = pl.ds(pl.multiple_of(owner * feat, feat), feat)
        return jnp.dot(hidden[...], wd[:, lanes_at], preferred_element_type=jnp.float32)

    def partial_sums(q):
        sib_out[q] = down(flip(owners[q], 1)).astype(jnp.bfloat16)
        send("sum_sib", q, sib_out.at[q], sib_in.at[q], {"tensor": sib})
        own_part[q] = down(owners[q])

    def chip_sum(q, s):
        at = group_rows(s)
        return own_part[q, at] + sib_in[q, at].astype(jnp.float32)

    def sum_d(s):
        d_out[s] = chip_sum(3, s).astype(jnp.bfloat16)
        send("sum_d", s, d_out.at[s], d_in.at[s], {"tensor": tx if s % 2 == 0 else ty})

    def sum_x(s):
        value = chip_sum(1, s)
        if s % 2 == 1:
            arrive("sum_d", s)
            value = value + d_in[s].astype(jnp.float32)
        x_out[s] = value.astype(jnp.bfloat16)
        send("sum_x", s, x_out.at[s], x_in.at[s], {"tensor": tx})

    def sum_y(s):
        value = chip_sum(2, s)
        if s % 2 == 0:
            arrive("sum_d", s)
            value = value + d_in[s].astype(jnp.float32)
        y_out[s] = value.astype(jnp.bfloat16)
        send("sum_y", s, y_out.at[s], y_in.at[s], {"tensor": ty})

    def total(s):
        arrive("sum_x", s)
        arrive("sum_y", s)
        value = chip_sum(0, s) + x_in[s].astype(jnp.float32) + y_in[s].astype(jnp.float32)
        return value.astype(jnp.bfloat16)

    def give_back(s):
        z_out[s] = total(s)
        send("back", s, z_out.at[s], z_in.at[pl.ds(s * cap, cap)], {"expert": group_of[s]})

    partial_sums(3)
    partial_sums(1)
    arrive("sum_sib", 3)
    sum_d(2)
    sum_d(3)
    partial_sums(2)
    arrive("sum_sib", 1)
    sum_x(2)
    arrive("sum_sib", 2)
    sum_y(3)
    sum_d(0)
    sum_d(1)
    partial_sums(0)
    sum_x(3)
    sum_y(2)
    sum_x(0)
    sum_y(1)
    arrive("sum_sib", 0)
    sum_x(1)
    sum_y(0)
    give_back(2)
    give_back(3)
    give_back(1)
    z_in[pl.ds(0, cap)] = total(0)

    weights = cw_ref[...]
    mixing = match0 * weights[0:1] + match1 * weights[1:2]
    coarse = mixing.astype(jnp.bfloat16)
    fine = (mixing - coarse.astype(jnp.float32)).astype(jnp.bfloat16)
    for s in (2, 3, 1):
        arrive("back", s)
    returned = z_in[...]
    combined = contract_first(coarse, returned) + contract_first(fine, returned)
    out_ref[...] = combined.astype(jnp.bfloat16)
    for copy in copies.values():
        copy.wait_send()


NAMES = (
    "z", "own_x", "own_y", "own_sib", "diag", "sib_x", "sib_y", "sib_d",
    "sum_sib", "sum_d", "sum_x", "sum_y", "back",
)


def fused_shards(stashed, expert_ids, combine_weight, w_gate, w_up, w_down):
    groups = lax.axis_size("expert")
    tokens, feat = stashed.shape
    cap = min(tokens, 8 * tokens // (3 * groups))
    _, units, width = w_gate.shape
    rows = groups * cap
    bf16, f32 = jnp.bfloat16, jnp.float32
    vmem = pl.BlockSpec(memory_space=pltpu.VMEM)
    hbm = pl.BlockSpec(memory_space=pl.ANY)
    pieces = [pltpu.VMEM((groups, cap, feat), bf16)] * 7
    return pl.pallas_call(
        functools.partial(layer_kernel, groups, cap),
        out_shape=jax.ShapeDtypeStruct((tokens, feat), bf16),
        in_specs=[vmem, vmem, vmem, hbm, hbm, hbm],
        out_specs=vmem,
        scratch_shapes=[
            pltpu.VMEM((units, width), bf16),
            pltpu.VMEM((units, width), bf16),
            pltpu.VMEM((units, width), bf16),
            pltpu.VMEM((rows, feat), bf16),
            pltpu.VMEM((width // (2 * feat), rows, 2 * feat), bf16),
            pltpu.VMEM((rows, units), f32),
            pltpu.VMEM((rows, units), f32),
            pltpu.VMEM((rows, units), bf16),
            pltpu.VMEM((4, rows, feat), bf16),
            pltpu.VMEM((4, rows, feat), bf16),
            pltpu.VMEM((4, rows, feat), f32),
            *pieces,
            pltpu.VMEM((rows, feat), bf16),
            pltpu.SemaphoreType.DMA((6,)),
            pltpu.SemaphoreType.DMA((len(NAMES) * groups,)),
            pltpu.SemaphoreType.DMA((len(NAMES) * groups,)),
        ],
        compiler_params=pltpu.CompilerParams(
            collective_id=0, has_side_effects=True, vmem_limit_bytes=60 * 1024 * 1024
        ),
    )(stashed, expert_ids.T, combine_weight.T, w_gate, w_up, w_down)


def picks_kernel(mesh):
    return mesh.shape["tensor"] == 8 and mesh.shape["expert"] == 4


def solution(mesh):
    return jax.shard_map(
        fused_shards if picks_kernel(mesh) else shards,
        mesh=mesh,
        in_specs=(
            P("expert", "tensor"),
            P("expert", None),
            P("expert", None),
            P("expert", "tensor", None),
            P("expert", "tensor", None),
            P("expert", "tensor", None),
        ),
        out_specs=P("expert", "tensor"),
        check_vma=False,
    )
```
